32 devices in a mesh: cell: 8 (over z, x), gene: 4 (over y, core).
Axes of the slice: x: 2, y: 2, z: 4, core: 2. Of those that a mesh axis runs over, the one named last changes fastest.
Arguments:
- counts: int32 [2048, 4096], P('cell', 'gene'), may hold values from 0 to 7
- totals: int32 [2048], P('cell'), may hold values from 1000 to 19999
- cell_factors: float32 [2048, 32], P('cell'), may hold values from -0.9 to 0.9
- gene_loadings: float32 [4096, 32], P('gene'), may hold values from -0.9 to 0.9
Outputs:
- new_factors: float32 [2048, 32], P('cell')
- new_loadings: float32 [4096, 32], P('gene')
- deviance: float32 [4096], P('gene')
The draws below stay inside these ranges and needn't reach their ends.
All inputs are finite; a program needn't handle non-finite values.
Results may differ from the reference program's by a relative error of at most 0.0044.
Values sent between devices are 32-bit elements; how exact they have to be, the bound alone decides.
A program may use at most 128 MiB of HBM per device.

```python
import math
import jax
import jax.numpy as jnp
from jax import lax

L = 32
GENES = 4096
CD = 256
CELLS = 2048
N_CELL = 8


def set_ends(result, rng, smallest, largest):
    shape = result.shape
    place = [jax.random.randint(jax.random.fold_in(rng, axis), (), 0, shape[axis]) for axis in range(len(shape))]
    result = result.at[tuple(place)].set(smallest)
    longest = shape.index(max(shape))
    place[longest] = (place[longest] + 1) % shape[longest]
    return result.at[tuple(place)].set(largest)


def block_levels(stream_key, shape, shards, smallest, top_value):
    gain = 1.0
    for dim, parts in shards:
        draws = jax.random.uniform(jax.random.fold_in(jax.random.fold_in(stream_key, 6), dim), (parts,), jnp.float32, smallest / len(shards), top_value / len(shards))
        gain = gain * jnp.repeat(jnp.exp(draws), shape[dim] // parts).reshape((-1,) + (1,) * (len(shape) - 1 - dim))
    return gain


def gaussian(rng, extent, deviation, bound, shards=(), dtype=jnp.bfloat16):
    result = deviation * jax.random.normal(rng, extent, jnp.float32)
    if shards:
        result = result * block_levels(rng, extent, shards, -0.22, 0.18)
    return jnp.clip(result, -bound, bound).astype(dtype)


def setup_inputs(seed: int = 0) -> dict:
    keys = jax.random.split(jax.random.key(seed), 5)
    counts = set_ends(jax.random.randint(keys[0], (CELLS, GENES), 0, 8), jax.random.fold_in(keys[0], 1), 0, 7).astype(jnp.int32)
    totals = set_ends(jax.random.randint(keys[1], (CELLS,), 1000, 20000), jax.random.fold_in(keys[1], 1), 1000, 19999).astype(jnp.int32)
    cell_factors = gaussian(keys[2], (CELLS, L), 0.15, 0.9, ((0, 8),), jnp.float32)
    gene_loadings = gaussian(keys[3], (GENES, L), 0.15, 0.9, ((0, 4),), jnp.float32)
    return {"counts": counts, "totals": totals, "cell_factors": cell_factors, "gene_loadings": gene_loadings}


RIDGE = 1.0
DAMPING = 0.1
SCALE_TOTAL = 5000.0

def outer_table(factors):
    width = factors.shape[1]
    product = factors[:, :, None] * factors[:, None, :]
    return product.reshape(factors.shape[0], width * width).astype(jnp.bfloat16)

def newton_solve(curvature, gradient):
    width = gradient.shape[1]
    matrix = jnp.transpose(curvature.reshape(gradient.shape[0], width, width), (1, 2, 0))
    diagonal_mean = sum((matrix[index, index] for index in range(width))) / width
    shift = RIDGE + DAMPING * diagonal_mean
    right = jnp.transpose(gradient)
    columns = []
    for column in range(width):
        current = matrix[:, column]
        if column > 0:
            stacked = jnp.stack(columns)
            current = current - lax.optimization_barrier(jnp.sum(stacked * stacked[:, column][:, None, :], axis=0))
        current = current + jnp.where(jnp.arange(width) == column, 1.0, 0.0).astype(jnp.float32)[:, None] * shift[None, :]
        pivot = jnp.sqrt(current[column])
        mask = (jnp.arange(width) >= column).astype(jnp.float32)[:, None]
        columns.append(mask * current / pivot[None, :])
    lower = jnp.stack(columns, axis=1)
    forward = []
    for row in range(width):
        value = right[row]
        for inner in range(row):
            value = value - lower[row, inner] * forward[inner]
        forward.append(value / lower[row, row])
    backward = [None] * width
    for row in range(width - 1, -1, -1):
        value = forward[row]
        for inner in range(row + 1, width):
            value = value - lower[inner, row] * backward[inner]
        backward[row] = value / lower[row, row]
    return jnp.transpose(jnp.stack(backward))

def predict(offset, factors, loadings):
    linear = offset[:, None] + jnp.dot(factors, loadings.T, precision=lax.Precision.HIGHEST)
    return (linear, jnp.exp(linear))

def gene_contract(counts, expected, loadings):
    weights = expected.astype(jnp.bfloat16)
    residual = (counts.astype(jnp.float32) - expected).astype(jnp.bfloat16)
    gradient = jnp.dot(residual, loadings.astype(jnp.bfloat16), preferred_element_type=jnp.float32)
    curvature = jnp.dot(weights, outer_table(loadings), preferred_element_type=jnp.float32)
    return (gradient, curvature)

def cell_contract(counts, linear, expected, factors):
    counts_real = counts.astype(jnp.float32)
    weights = expected.astype(jnp.bfloat16)
    residual = (counts_real - expected).astype(jnp.bfloat16)
    dims = (((0,), (0,)), ((), ()))
    gradient = lax.dot_general(residual, factors.astype(jnp.bfloat16), dims, preferred_element_type=jnp.float32)
    curvature = lax.dot_general(weights, outer_table(factors), dims, preferred_element_type=jnp.float32)
    terms = 2.0 * (counts_real * (jnp.log(jnp.maximum(counts_real, 1.0)) - linear) - counts_real + expected)
    return (gradient, curvature, lax.optimization_barrier(jnp.sum(terms, axis=0)))

def reference(counts, totals, cell_factors, gene_loadings):
    offset = jnp.log(totals.astype(jnp.float32)) - math.log(SCALE_TOTAL)
    count_blocks = counts.reshape(N_CELL, CD, GENES)
    offset_blocks = offset.reshape(N_CELL, CD)
    factor_blocks = cell_factors.reshape(N_CELL, CD, L)

    def factor_update(block):
        count_block, offset_block, factor_block = block
        linear, expected = predict(offset_block, factor_block, gene_loadings)
        gradient, curvature = gene_contract(count_block, expected, gene_loadings)
        return factor_block + newton_solve(curvature, gradient - RIDGE * factor_block)
    new_blocks = lax.map(factor_update, (count_blocks, offset_blocks, factor_blocks))
    new_factors = new_blocks.reshape(CELLS, L)

    def loading_update(running, block):
        count_block, offset_block, factor_block = block
        linear, expected = predict(offset_block, factor_block, gene_loadings)
        gradient, curvature, deviance_part = cell_contract(count_block, linear, expected, factor_block)
        return ((running[0] + gradient, running[1] + curvature, running[2] + deviance_part), None)
    initial = (jnp.zeros((GENES, L), jnp.float32), jnp.zeros((GENES, L * L), jnp.float32), jnp.zeros((GENES,), jnp.float32))
    totals_sum, unused = lax.scan(loading_update, initial, (count_blocks, offset_blocks, new_blocks))
    gradient_sum, curvature_sum, deviance_sum = totals_sum
    new_loadings = gene_loadings + newton_solve(curvature_sum, gradient_sum - RIDGE * gene_loadings)
    deviance = deviance_sum / CELLS
    return (new_factors, new_loadings, deviance)
```

```python
import functools
import math

import jax
import jax.numpy as jnp
from jax import lax
from jax.experimental import pallas as pl
from jax.experimental.pallas import tpu as pltpu
from jax.sharding import PartitionSpec as P

RIDGE = 1.0
DAMPING = 0.1
SCALE_TOTAL = 5000.0
LANES = 128
SUB = 8
BLOCK = 256
HIGH = lax.Precision.HIGHEST
NT = (((1,), (1,)), ((), ()))
F32 = jnp.float32
BF16 = jnp.bfloat16


def packed_rows(width):
    return sum(width - SUB * (a // SUB) for a in range(width))


def lower_table(factors):
    width = factors.shape[0]
    pieces = [factors[a : a + 1] * factors[SUB * (a // SUB) :] for a in range(width)]
    return jnp.concatenate(pieces, axis=0).astype(BF16)


def solve_packed(get, right, width):
    blocks, start = [], 0
    for block in range(width // SUB):
        rows = width - SUB * block
        blocks.append(get(start, SUB * rows).reshape(SUB, rows, right.shape[1]))
        start += SUB * rows
    diagonal = sum(blocks[a // SUB][a % SUB, a % SUB : a % SUB + 1] for a in range(width)) / width
    shift = RIDGE + DAMPING * diagonal
    count = width // SUB
    index = lax.broadcasted_iota(jnp.int32, (width, right.shape[1]), 0)
    lower, scaled = [], []
    value = right
    for a in range(width):
        own, place = a // SUB, a % SUB
        column = blocks[own][place]
        rows = index[: width - SUB * own]
        inverse = 1.0 / (column[place : place + 1] + shift)
        factor = jnp.where(rows > place, column * inverse, 0.0)
        for block in range(own, count):
            offset = SUB * (block - own)
            coefficient = column[offset : offset + SUB]
            blocks[block] = blocks[block] - factor[offset:][None] * coefficient[:, None, :]
        lower.append(factor)
        head = value[SUB * own :]
        pivot = head[place : place + 1]
        scaled.append(pivot * inverse)
        head = head - factor * pivot
        value = head if own == 0 else jnp.concatenate([value[: SUB * own], head], axis=0)
    parts = [None] * count
    for a in range(width - 1, -1, -1):
        own, place = a // SUB, a % SUB
        rows = index[:SUB]
        if parts[own] is None:
            parts[own] = jnp.zeros((SUB, right.shape[1]), F32)
        known = jnp.concatenate(parts[own:], axis=0)
        found = scaled[a] - jnp.sum(lower[a] * known, axis=0, keepdims=True)
        parts[own] = jnp.where(rows == place, found, parts[own])
    return jnp.concatenate(parts, axis=0)


def solve_kernel(width, curvature_ref, gradient_ref, out_ref):
    out_ref[...] = solve_packed(
        lambda start, rows: curvature_ref[start : start + rows], gradient_ref[...], width
    )


def newton_solve(curvature, gradient):
    count, width = gradient.shape
    matrix = jnp.transpose(curvature).reshape(width, width, count)
    packed = jnp.concatenate([matrix[a, SUB * (a // SUB) :] for a in range(width)], axis=0)
    fill = -count % LANES
    packed = jnp.pad(packed, ((0, 0), (0, fill)))
    right = jnp.pad(jnp.transpose(gradient), ((0, 0), (0, fill)))
    rows = packed.shape[0]
    result = pl.pallas_call(
        functools.partial(solve_kernel, width),
        grid=((count + fill) // LANES,),
        in_specs=[
            pl.BlockSpec((rows, LANES), lambda i: (0, i)),
            pl.BlockSpec((width, LANES), lambda i: (0, i)),
        ],
        out_specs=pl.BlockSpec((width, LANES), lambda i: (0, i)),
        out_shape=jax.ShapeDtypeStruct(right.shape, F32),
    )(packed, right)
    return jnp.transpose(result[:, :count])


def outer_table(factors):
    width = factors.shape[1]
    product = factors[:, :, None] * factors[:, None, :]
    return product.reshape(factors.shape[0], width * width).astype(BF16)


def predict(offset, factors, loadings):
    linear = offset[:, None] + jnp.dot(factors, loadings.T, precision=HIGH)
    return (linear, jnp.exp(linear))


def gene_contract(counts, expected, loadings):
    weights = expected.astype(BF16)
    residual = (counts.astype(F32) - expected).astype(BF16)
    gradient = jnp.dot(residual, loadings.astype(BF16), preferred_element_type=F32)
    curvature = jnp.dot(weights, outer_table(loadings), preferred_element_type=F32)
    return (gradient, curvature)


def cell_contract(counts, linear, expected, factors):
    counts_real = counts.astype(F32)
    weights = expected.astype(BF16)
    residual = (counts_real - expected).astype(BF16)
    dims = (((0,), (0,)), ((), ()))
    gradient = lax.dot_general(residual, factors.astype(BF16), dims, preferred_element_type=F32)
    curvature = lax.dot_general(weights, outer_table(factors), dims, preferred_element_type=F32)
    terms = 2.0 * (
        counts_real * (jnp.log(jnp.maximum(counts_real, 1.0)) - linear) - counts_real + expected
    )
    return (gradient, curvature, jnp.sum(terms, axis=0))


def by_collectives(counts, totals, cell_factors, gene_loadings):
    offset = jnp.log(totals.astype(F32)) - math.log(SCALE_TOTAL)
    linear, expected = predict(offset, cell_factors, gene_loadings)
    gradient_part, curvature_part = gene_contract(counts, expected, gene_loadings)
    gradient_sum, curvature_sum = lax.psum((gradient_part, curvature_part), "gene")
    new_factors = cell_factors + newton_solve(curvature_sum, gradient_sum - RIDGE * cell_factors)
    cell_total = counts.shape[0] * lax.axis_size("cell")
    linear_next, expected_next = predict(offset, new_factors, gene_loadings)
    gradient_part, curvature_part, deviance_part = cell_contract(
        counts, linear_next, expected_next, new_factors
    )
    gradient_share, curvature_share, deviance_share = (
        lax.psum_scatter(gradient_part, "cell", scatter_dimension=0, tiled=True),
        lax.psum_scatter(curvature_part, "cell", scatter_dimension=0, tiled=True),
        lax.psum_scatter(deviance_part, "cell", scatter_dimension=0, tiled=True),
    )
    portion = gradient_share.shape[0]
    start_row = lax.axis_index("cell") * portion
    own_rows = lax.dynamic_slice_in_dim(gene_loadings, start_row, portion, 0)
    own_new = own_rows + newton_solve(curvature_share, gradient_share - RIDGE * own_rows)
    new_loadings, deviance = (
        lax.all_gather(own_new, "cell", axis=0, tiled=True),
        lax.all_gather(deviance_share / cell_total, "cell", axis=0, tiled=True),
    )
    return (new_factors, new_loadings, deviance)


def extended(rows, last):
    n = rows.shape[1]
    index = lax.broadcasted_iota(jnp.int32, (SUB, n), 0)
    return jnp.concatenate([rows, jnp.where(index == 0, last, 0.0)], axis=0)


def send(source, target, send_sem, recv_sem, device):
    return pltpu.make_async_remote_copy(
        src_ref=source,
        dst_ref=target,
        send_sem=send_sem,
        recv_sem=recv_sem,
        device_id=device,
        device_id_type=pl.DeviceIdType.MESH,
    )


def sweep_kernel(
    n_cell,
    n_gene,
    counts_ref,
    totals_ref,
    factors_ref,
    loadings_ref,
    new_factors_ref,
    new_loadings_ref,
    deviance_ref,
    all_counts,
    all_totals,
    total,
    share,
    arrived,
    own_factors,
    all_factors,
    sums,
    dev_sum,
    own_loadings,
    all_loadings,
    counts_out,
    counts_in,
    totals_out,
    totals_in,
    share_out,
    share_in,
    factors_out,
    factors_in,
    loadings_out,
    loadings_in,
):
    cell, gene = lax.axis_index("cell"), lax.axis_index("gene")
    cells, width = factors_ref.shape
    genes = loadings_ref.shape[0]
    devices = n_cell * n_gene
    half = LANES // 2
    me = cell * n_gene + gene

    def device(step):
        other = lax.rem(me + step, devices)
        return {"cell": other // n_gene, "gene": lax.rem(other, n_gene)}

    barrier = pltpu.get_barrier_semaphore()

    @pl.loop(1, devices)
    def _(step):
        pl.semaphore_signal(
            barrier, inc=1, device_id=device(step), device_id_type=pl.DeviceIdType.MESH
        )

    pl.semaphore_wait(barrier, devices - 1)

    early = []
    for step in range(1, n_cell):
        other = lax.rem(cell + step, n_cell)
        columns = pl.ds(pl.multiple_of(other * LANES, LANES), LANES)
        there = {"cell": other, "gene": gene}
        early.append(
            send(counts_ref.at[:, columns], all_counts.at[cell], counts_out.at[step], counts_in.at[step], there)
        )
        early.append(
            send(totals_ref, all_totals.at[cell], totals_out.at[step], totals_in.at[step], there)
        )
    for copy in early:
        copy.start()
    own_columns = pl.ds(pl.multiple_of(cell * LANES, LANES), LANES)
    all_counts[cell] = counts_ref[:, own_columns]
    all_totals[cell] = totals_ref[...]

    offset = jnp.log(totals_ref[...].astype(F32)) - math.log(SCALE_TOTAL)
    left = jnp.transpose(extended(jnp.transpose(factors_ref[...]), offset))
    total[...] = jnp.zeros_like(total)

    @pl.loop(0, genes // BLOCK)
    def _(block):
        where = pl.ds(pl.multiple_of(block * BLOCK, BLOCK), BLOCK)
        rows = jnp.transpose(loadings_ref[where, :])
        expected = jnp.exp(jnp.dot(left, extended(rows, 1.0), precision=HIGH, preferred_element_type=F32))
        weights = expected.astype(BF16)
        residual = (counts_ref[:, where].astype(F32) - expected).astype(BF16)
        total[:width] += lax.dot_general(rows.astype(BF16), residual, NT, preferred_element_type=F32)
        total[width:] += lax.dot_general(lower_table(rows), weights, NT, preferred_element_type=F32)

    size = total.shape[0] // 2
    lane = lax.broadcasted_iota(jnp.int32, (size, LANES), 1)
    for pair in range(n_gene // 2):
        columns = slice(pair * LANES, (pair + 1) * LANES)
        top, bottom = total[:size, columns], total[size:, columns]
        share[2 * pair] = jnp.where(lane < half, top, pltpu.roll(bottom, half, 1))
        share[2 * pair + 1] = jnp.where(lane < half, pltpu.roll(top, half, 1), bottom)
    shares = []
    for step in range(1, n_gene):
        other = lax.rem(gene + step, n_gene)
        there = {"cell": cell, "gene": other}
        shares.append(
            send(share.at[other], arrived.at[step], share_out.at[step], share_in.at[step], there)
        )
    for copy in shares:
        copy.start()
    own_rows = factors_ref[pl.ds(pl.multiple_of(gene * half, half), half), :]
    own_rows = jnp.transpose(jnp.concatenate([own_rows, own_rows], axis=0))
    for copy in shares:
        copy.wait()
    both = share[gene]
    for step in range(1, n_gene):
        both = both + arrived[step]
    sums[:size] = both
    sums[size:] = pltpu.roll(both, half, 1)
    found = own_rows + solve_packed(
        lambda start, rows: sums[width + start : width + start + rows],
        sums[:width] - RIDGE * own_rows,
        width,
    )
    lane = lax.broadcasted_iota(jnp.int32, (width // 2, LANES), 1)
    packed = jnp.where(lane < half, found[: width // 2], pltpu.roll(found[width // 2 :], half, 1))
    own_factors[...] = packed
    all_factors[me] = packed

    def factors_copy(step):
        return send(own_factors, all_factors.at[me], factors_out.at[step], factors_in.at[step], device(step))

    @pl.loop(1, devices)
    def _(step):
        factors_copy(step).start()

    own_genes = pl.ds(pl.multiple_of(cell * LANES, LANES), LANES)
    own_loadings_rows = jnp.transpose(loadings_ref[own_genes, :])
    right = extended(own_loadings_rows, 1.0)
    sums[...] = jnp.zeros_like(sums)
    dev_sum[...] = jnp.zeros_like(dev_sum)
    for copy in early:
        copy.wait()

    @pl.loop(1, devices)
    def _(step):
        factors_copy(step).wait()

    def cell_rows(index):
        tiles = []
        for pair in range(n_gene // 2):
            first = all_factors[index * n_gene + 2 * pair]
            second = all_factors[index * n_gene + 2 * pair + 1]
            top = jnp.where(lane < half, first, pltpu.roll(second, half, 1))
            bottom = jnp.where(lane < half, pltpu.roll(first, half, 1), second)
            tiles.append(jnp.concatenate([top, bottom], axis=0))
        return jnp.concatenate(tiles, axis=1)

    @pl.loop(0, n_cell)
    def _(index):
        rows = cell_rows(index)
        offsets = jnp.log(all_totals[index].astype(F32)) - math.log(SCALE_TOTAL)
        linear = jnp.dot(
            jnp.transpose(extended(rows, offsets)), right, precision=HIGH, preferred_element_type=F32
        )
        expected = jnp.exp(linear)
        real = all_counts[index].astype(F32)
        weights = expected.astype(BF16)
        residual = (real - expected).astype(BF16)
        sums[:width] += jnp.dot(rows.astype(BF16), residual, preferred_element_type=F32)
        sums[width:] += jnp.dot(lower_table(rows), weights, preferred_element_type=F32)
        terms = 2.0 * (real * (jnp.log(jnp.maximum(real, 1.0)) - linear) - real + expected)
        dev_sum[...] += jnp.sum(terms, axis=0, keepdims=True)

    new_rows = own_loadings_rows + solve_packed(
        lambda start, rows: sums[width + start : width + start + rows],
        sums[:width] - RIDGE * own_loadings_rows,
        width,
    )
    result = extended(new_rows, dev_sum[...] / (cells * n_cell))
    own_loadings[...] = result
    all_loadings[cell] = result
    last = []
    for step in range(1, n_cell):
        other = lax.rem(cell + step, n_cell)
        there = {"cell": other, "gene": gene}
        last.append(
            send(own_loadings, all_loadings.at[cell], loadings_out.at[step], loadings_in.at[step], there)
        )
    for copy in last:
        copy.start()
    new_factors_ref[...] = jnp.transpose(cell_rows(cell))
    for copy in last:
        copy.wait()
    for index in range(n_cell):
        block = all_loadings[index]
        new_loadings_ref[index * LANES : (index + 1) * LANES, :] = jnp.transpose(block[:width])
        deviance_ref[:, index * LANES : (index + 1) * LANES] = block[width : width + 1]


def by_kernel(n_cell, n_gene, counts, totals, cell_factors, gene_loadings):
    cells, genes = counts.shape
    width = cell_factors.shape[1]
    rows = width + packed_rows(width)
    devices = n_cell * n_gene
    vmem = pl.BlockSpec(memory_space=pltpu.VMEM)
    dma = lambda n: pltpu.SemaphoreType.DMA((n,))
    new_factors, new_loadings, deviance = pl.pallas_call(
        functools.partial(sweep_kernel, n_cell, n_gene),
        out_shape=(
            jax.ShapeDtypeStruct((cells, width), F32),
            jax.ShapeDtypeStruct((genes, width), F32),
            jax.ShapeDtypeStruct((1, genes), F32),
        ),
        in_specs=[vmem] * 4,
        out_specs=(vmem,) * 3,
        scratch_shapes=[
            pltpu.VMEM((n_cell, cells, LANES), jnp.int32),
            pltpu.VMEM((n_cell, 1, cells), jnp.int32),
            pltpu.VMEM((rows, cells), F32),
            pltpu.VMEM((n_gene, rows // 2, LANES), F32),
            pltpu.VMEM((n_gene, rows // 2, LANES), F32),
            pltpu.VMEM((width // 2, LANES), F32),
            pltpu.VMEM((devices, width // 2, LANES), F32),
            pltpu.VMEM((rows, LANES), F32),
            pltpu.VMEM((1, LANES), F32),
            pltpu.VMEM((width + SUB, LANES), F32),
            pltpu.VMEM((n_cell, width + SUB, LANES), F32),
            dma(n_cell),
            dma(n_cell),
            dma(n_cell),
            dma(n_cell),
            dma(n_gene),
            dma(n_gene),
            dma(devices),
            dma(devices),
            dma(n_cell),
            dma(n_cell),
        ],
        compiler_params=pltpu.CompilerParams(
            collective_id=0, has_side_effects=True, vmem_limit_bytes=48 * 1024 * 1024
        ),
    )(counts, totals.reshape(1, cells), cell_factors, gene_loadings)
    return (new_factors, new_loadings, deviance.reshape(genes))


def solution(mesh):
    n_cell, n_gene = mesh.shape["cell"], mesh.shape["gene"]

    def on_device(counts, totals, cell_factors, gene_loadings):
        cells, genes = counts.shape
        whole_lanes = genes == n_cell * LANES and 2 * cells == n_gene * LANES
        if whole_lanes and n_gene % 2 == 0 and genes % BLOCK == 0:
            return by_kernel(n_cell, n_gene, counts, totals, cell_factors, gene_loadings)
        return by_collectives(counts, totals, cell_factors, gene_loadings)

    return jax.shard_map(
        on_device,
        mesh=mesh,
        in_specs=(P("cell", "gene"), P("cell"), P("cell", None), P("gene", None)),
        out_specs=(P("cell", None), P("gene", None), P("gene")),
        check_vma=False,
    )
```

```python
import functools
import math

import jax
import jax.numpy as jnp
from jax import lax
from jax.experimental import pallas as pl
from jax.experimental.pallas import tpu as pltpu
from jax.sharding import PartitionSpec as P

RIDGE = 1.0
DAMPING = 0.1
SCALE_TOTAL = 5000.0
LANES = 128
SUB = 8
BLOCK = 256
HIGH = lax.Precision.HIGHEST
NT = (((1,), (1,)), ((), ()))
F32 = jnp.float32
BF16 = jnp.bfloat16


def packed_rows(width):
    return sum(width - SUB * (a // SUB) for a in range(width))


def lower_table(factors):
    width = factors.shape[0]
    pieces = [factors[a : a + 1] * factors[SUB * (a // SUB) :] for a in range(width)]
    return jnp.concatenate(pieces, axis=0).astype(BF16)


def solve_packed(get, right, width):
    blocks, start = [], 0
    for block in range(width // SUB):
        rows = width - SUB * block
        blocks.append(get(start, SUB * rows).reshape(SUB, rows, right.shape[1]))
        start += SUB * rows
    diagonal = sum(blocks[a // SUB][a % SUB, a % SUB : a % SUB + 1] for a in range(width)) / width
    shift = RIDGE + DAMPING * diagonal
    count = width // SUB
    index = lax.broadcasted_iota(jnp.int32, (width, right.shape[1]), 0)
    lower, scaled = [], []
    value = right
    for a in range(width):
        own, place = a // SUB, a % SUB
        column = blocks[own][place]
        rows = index[: width - SUB * own]
        inverse = 1.0 / (column[place : place + 1] + shift)
        factor = jnp.where(rows > place, column * inverse, 0.0)
        for block in range(own, count):
            offset = SUB * (block - own)
            coefficient = column[offset : offset + SUB]
            blocks[block] = blocks[block] - factor[offset:][None] * coefficient[:, None, :]
        lower.append(factor)
        head = value[SUB * own :]
        pivot = head[place : place + 1]
        scaled.append(pivot * inverse)
        head = head - factor * pivot
        value = head if own == 0 else jnp.concatenate([value[: SUB * own], head], axis=0)
    parts = [None] * count
    for a in range(width - 1, -1, -1):
        own, place = a // SUB, a % SUB
        rows = index[:SUB]
        if parts[own] is None:
            parts[own] = jnp.zeros((SUB, right.shape[1]), F32)
        known = jnp.concatenate(parts[own:], axis=0)
        found = scaled[a] - jnp.sum(lower[a] * known, axis=0, keepdims=True)
        parts[own] = jnp.where(rows == place, found, parts[own])
    return jnp.concatenate(parts, axis=0)


def solve_kernel(width, curvature_ref, gradient_ref, out_ref):
    out_ref[...] = solve_packed(
        lambda start, rows: curvature_ref[start : start + rows], gradient_ref[...], width
    )


def newton_solve(curvature, gradient):
    count, width = gradient.shape
    matrix = jnp.transpose(curvature).reshape(width, width, count)
    packed = jnp.concatenate([matrix[a, SUB * (a // SUB) :] for a in range(width)], axis=0)
    fill = -count % LANES
    packed = jnp.pad(packed, ((0, 0), (0, fill)))
    right = jnp.pad(jnp.transpose(gradient), ((0, 0), (0, fill)))
    rows = packed.shape[0]
    result = pl.pallas_call(
        functools.partial(solve_kernel, width),
        grid=((count + fill) // LANES,),
        in_specs=[
            pl.BlockSpec((rows, LANES), lambda i: (0, i)),
            pl.BlockSpec((width, LANES), lambda i: (0, i)),
        ],
        out_specs=pl.BlockSpec((width, LANES), lambda i: (0, i)),
        out_shape=jax.ShapeDtypeStruct(right.shape, F32),
    )(packed, right)
    return jnp.transpose(result[:, :count])


def outer_table(factors):
    width = factors.shape[1]
    product = factors[:, :, None] * factors[:, None, :]
    return product.reshape(factors.shape[0], width * width).astype(BF16)


def predict(offset, factors, loadings):
    linear = offset[:, None] + jnp.dot(factors, loadings.T, precision=HIGH)
    return (linear, jnp.exp(linear))


def gene_contract(counts, expected, loadings):
    weights = expected.astype(BF16)
    residual = (counts.astype(F32) - expected).astype(BF16)
    gradient = jnp.dot(residual, loadings.astype(BF16), preferred_element_type=F32)
    curvature = jnp.dot(weights, outer_table(loadings), preferred_element_type=F32)
    return (gradient, curvature)


def cell_contract(counts, linear, expected, factors):
    counts_real = counts.astype(F32)
    weights = expected.astype(BF16)
    residual = (counts_real - expected).astype(BF16)
    dims = (((0,), (0,)), ((), ()))
    gradient = lax.dot_general(residual, factors.astype(BF16), dims, preferred_element_type=F32)
    curvature = lax.dot_general(weights, outer_table(factors), dims, preferred_element_type=F32)
    terms = 2.0 * (
        counts_real * (jnp.log(jnp.maximum(counts_real, 1.0)) - linear) - counts_real + expected
    )
    return (gradient, curvature, jnp.sum(terms, axis=0))


def by_collectives(counts, totals, cell_factors, gene_loadings):
    offset = jnp.log(totals.astype(F32)) - math.log(SCALE_TOTAL)
    linear, expected = predict(offset, cell_factors, gene_loadings)
    gradient_part, curvature_part = gene_contract(counts, expected, gene_loadings)
    gradient_sum, curvature_sum = lax.psum((gradient_part, curvature_part), "gene")
    new_factors = cell_factors + newton_solve(curvature_sum, gradient_sum - RIDGE * cell_factors)
    cell_total = counts.shape[0] * lax.axis_size("cell")
    linear_next, expected_next = predict(offset, new_factors, gene_loadings)
    gradient_part, curvature_part, deviance_part = cell_contract(
        counts, linear_next, expected_next, new_factors
    )
    gradient_share, curvature_share, deviance_share = (
        lax.psum_scatter(gradient_part, "cell", scatter_dimension=0, tiled=True),
        lax.psum_scatter(curvature_part, "cell", scatter_dimension=0, tiled=True),
        lax.psum_scatter(deviance_part, "cell", scatter_dimension=0, tiled=True),
    )
    portion = gradient_share.shape[0]
    start_row = lax.axis_index("cell") * portion
    own_rows = lax.dynamic_slice_in_dim(gene_loadings, start_row, portion, 0)
    own_new = own_rows + newton_solve(curvature_share, gradient_share - RIDGE * own_rows)
    new_loadings, deviance = (
        lax.all_gather(own_new, "cell", axis=0, tiled=True),
        lax.all_gather(deviance_share / cell_total, "cell", axis=0, tiled=True),
    )
    return (new_factors, new_loadings, deviance)


def extended(rows, last):
    n = rows.shape[1]
    index = lax.broadcasted_iota(jnp.int32, (SUB, n), 0)
    return jnp.concatenate([rows, jnp.where(index == 0, last, 0.0)], axis=0)


def send(source, target, send_sem, recv_sem, device):
    return pltpu.make_async_remote_copy(
        src_ref=source,
        dst_ref=target,
        send_sem=send_sem,
        recv_sem=recv_sem,
        device_id=device,
        device_id_type=pl.DeviceIdType.MESH,
    )


def sweep_kernel(
    n_cell,
    n_gene,
    counts_hbm,
    totals_ref,
    factors_ref,
    loadings_ref,
    new_factors_ref,
    new_loadings_ref,
    deviance_ref,
    counts_ref,
    all_counts,
    all_totals,
    total,
    share,
    arrived,
    own_factors,
    all_factors,
    sums,
    dev_sum,
    own_loadings,
    all_loadings,
    counts_out,
    counts_in,
    totals_out,
    totals_in,
    share_out,
    share_in,
    factors_out,
    factors_in,
    loadings_out,
    loadings_in,
    local_sem,
):
    cell, gene = lax.axis_index("cell"), lax.axis_index("gene")
    width, cells = factors_ref.shape
    genes = loadings_ref.shape[1]
    devices = n_cell * n_gene
    half = LANES // 2
    me = cell * n_gene + gene

    def device(cell_step, gene_step):
        return {"cell": lax.rem(cell + cell_step, n_cell), "gene": lax.rem(gene + gene_step, n_gene)}

    local = pltpu.make_async_copy(counts_hbm, counts_ref, local_sem)
    local.start()

    barrier = pltpu.get_barrier_semaphore()

    @pl.loop(1, devices)
    def _(step):
        pl.semaphore_signal(
            barrier, inc=1, device_id=device(step // n_gene, lax.rem(step, n_gene)), device_id_type=pl.DeviceIdType.MESH
        )

    pl.semaphore_wait(barrier, devices - 1)

    def counts_copy(step):
        other = lax.rem(cell + step, n_cell)
        columns = pl.ds(pl.multiple_of(other * LANES, LANES), LANES)
        return send(
            counts_hbm.at[:, columns],
            all_counts.at[cell],
            counts_out.at[step],
            counts_in.at[step],
            device(step, 0),
        )

    def totals_copy(step):
        return send(
            totals_ref, all_totals.at[cell], totals_out.at[step], totals_in.at[step], device(step, 0)
        )

    near_first = []
    for step in range(1, n_cell // 2 + 1):
        near_first += [step] if 2 * step == n_cell else [step, n_cell - step]
    for step in near_first[::-1]:
        counts_copy(step).start()
        totals_copy(step).start()
    own_columns = pl.ds(pl.multiple_of(cell * LANES, LANES), LANES)
    all_totals[cell] = totals_ref[...]
    local.wait()
    all_counts[cell] = counts_ref[:, own_columns]

    offset = jnp.log(totals_ref[...].astype(F32)) - math.log(SCALE_TOTAL)
    left = jnp.transpose(extended(factors_ref[...], offset))
    total[...] = jnp.zeros_like(total)

    @pl.loop(0, genes // BLOCK)
    def _(block):
        where = pl.ds(pl.multiple_of(block * BLOCK, BLOCK), BLOCK)
        rows = loadings_ref[:, where]
        expected = jnp.exp(jnp.dot(left, extended(rows, 1.0), precision=HIGH, preferred_element_type=F32))
        weights = expected.astype(BF16)
        residual = (counts_ref[:, where].astype(F32) - expected).astype(BF16)
        total[:width] += lax.dot_general(rows.astype(BF16), residual, NT, preferred_element_type=F32)
        total[width:] += lax.dot_general(lower_table(rows), weights, NT, preferred_element_type=F32)

    size = total.shape[0] // 2
    lane = lax.broadcasted_iota(jnp.int32, (size, LANES), 1)
    for pair in range(n_gene // 2):
        columns = slice(pair * LANES, (pair + 1) * LANES)
        top, bottom = total[:size, columns], total[size:, columns]
        share[2 * pair] = jnp.where(lane < half, top, pltpu.roll(bottom, half, 1))
        share[2 * pair + 1] = jnp.where(lane < half, pltpu.roll(top, half, 1), bottom)
    shares = []
    for step in range(1, n_gene):
        other = lax.rem(gene + step, n_gene)
        there = {"cell": cell, "gene": other}
        shares.append(
            send(share.at[other], arrived.at[step], share_out.at[step], share_in.at[step], there)
        )
    for copy in shares:
        copy.start()
    pair_columns = pl.ds(pl.multiple_of(gene // 2 * LANES, LANES), LANES)
    own_rows = pltpu.roll(factors_ref[:, pair_columns], half * lax.rem(gene, 2), 1)
    for copy in shares:
        copy.wait()
    both = share[gene]
    for step in range(1, n_gene):
        both = both + arrived[step]
    sums[:size] = both
    sums[size:] = pltpu.roll(both, half, 1)
    found = own_rows + solve_packed(
        lambda start, rows: sums[width + start : width + start + rows],
        sums[:width] - RIDGE * own_rows,
        width,
    )
    lane = lax.broadcasted_iota(jnp.int32, (width // 2, LANES), 1)
    packed = jnp.where(lane < half, found[: width // 2], pltpu.roll(found[width // 2 :], half, 1))
    own_factors[...] = packed
    all_factors[me] = packed

    def factors_copy(cell_step, gene_step):
        index = cell_step * n_gene + gene_step
        return send(
            own_factors,
            all_factors.at[me],
            factors_out.at[index],
            factors_in.at[index],
            device(cell_step, gene_step),
        )

    for cell_step in near_first[::-1] + [0]:
        for gene_step in range(n_gene):
            if cell_step + gene_step:
                factors_copy(cell_step, gene_step).start()

    own_loadings_rows = loadings_ref[:, own_columns]
    right = extended(own_loadings_rows, 1.0)
    sums[...] = jnp.zeros_like(sums)
    dev_sum[...] = jnp.zeros_like(dev_sum)

    def cell_rows(index):
        tiles = []
        for pair in range(n_gene // 2):
            first = all_factors[index * n_gene + 2 * pair]
            second = all_factors[index * n_gene + 2 * pair + 1]
            top = jnp.where(lane < half, first, pltpu.roll(second, half, 1))
            bottom = jnp.where(lane < half, pltpu.roll(first, half, 1), second)
            tiles.append(jnp.concatenate([top, bottom], axis=0))
        return jnp.concatenate(tiles, axis=1)

    def add_cells(index):
        rows = cell_rows(index)
        offsets = jnp.log(all_totals[index].astype(F32)) - math.log(SCALE_TOTAL)
        linear = jnp.dot(
            jnp.transpose(extended(rows, offsets)), right, precision=HIGH, preferred_element_type=F32
        )
        expected = jnp.exp(linear)
        real = all_counts[index].astype(F32)
        weights = expected.astype(BF16)
        residual = (real - expected).astype(BF16)
        sums[:width] += jnp.dot(rows.astype(BF16), residual, preferred_element_type=F32)
        sums[width:] += jnp.dot(lower_table(rows), weights, preferred_element_type=F32)
        terms = 2.0 * (real * (jnp.log(jnp.maximum(real, 1.0)) - linear) - real + expected)
        dev_sum[...] += jnp.sum(terms, axis=0, keepdims=True)

    for gene_step in range(1, n_gene):
        factors_copy(0, gene_step).wait()
    new_factors_ref[...] = cell_rows(cell)
    add_cells(cell)

    @pl.loop(1, n_cell)
    def _(place):
        odd = lax.rem(place, 2)
        step = odd * ((place + 1) // 2) + (1 - odd) * (n_cell - place // 2)
        counts_copy(step).wait()
        totals_copy(step).wait()
        for gene_step in range(n_gene):
            factors_copy(step, gene_step).wait()
        add_cells(lax.rem(cell + n_cell - step, n_cell))

    new_rows = own_loadings_rows + solve_packed(
        lambda start, rows: sums[width + start : width + start + rows],
        sums[:width] - RIDGE * own_loadings_rows,
        width,
    )
    result = extended(new_rows, dev_sum[...] / (cells * n_cell))
    own_loadings[...] = result
    all_loadings[cell] = result
    last = []
    for step in near_first[::-1]:
        there = device(step, 0)
        last.append(
            send(own_loadings, all_loadings.at[cell], loadings_out.at[step], loadings_in.at[step], there)
        )
    for copy in last:
        copy.start()
    for copy in last:
        copy.wait()
    for index in range(n_cell):
        block = all_loadings[index]
        new_loadings_ref[:, index * LANES : (index + 1) * LANES] = block[:width]
        deviance_ref[:, index * LANES : (index + 1) * LANES] = block[width : width + 1]


def by_kernel(n_cell, n_gene, counts, totals, cell_factors, gene_loadings):
    cells, genes = counts.shape
    width = cell_factors.shape[1]
    rows = width + packed_rows(width)
    devices = n_cell * n_gene
    vmem = pl.BlockSpec(memory_space=pltpu.VMEM)
    dma = lambda n: pltpu.SemaphoreType.DMA((n,))
    new_factors, new_loadings, deviance = pl.pallas_call(
        functools.partial(sweep_kernel, n_cell, n_gene),
        out_shape=(
            jax.ShapeDtypeStruct((width, cells), F32),
            jax.ShapeDtypeStruct((width, genes), F32),
            jax.ShapeDtypeStruct((1, genes), F32),
        ),
        in_specs=[pl.BlockSpec(memory_space=pl.ANY)] + [vmem] * 3,
        out_specs=(vmem,) * 3,
        scratch_shapes=[
            pltpu.VMEM((cells, genes), jnp.int32),
            pltpu.VMEM((n_cell, cells, LANES), jnp.int32),
            pltpu.VMEM((n_cell, 1, cells), jnp.int32),
            pltpu.VMEM((rows, cells), F32),
            pltpu.VMEM((n_gene, rows // 2, LANES), F32),
            pltpu.VMEM((n_gene, rows // 2, LANES), F32),
            pltpu.VMEM((width // 2, LANES), F32),
            pltpu.VMEM((devices, width // 2, LANES), F32),
            pltpu.VMEM((rows, LANES), F32),
            pltpu.VMEM((1, LANES), F32),
            pltpu.VMEM((width + SUB, LANES), F32),
            pltpu.VMEM((n_cell, width + SUB, LANES), F32),
            dma(n_cell),
            dma(n_cell),
            dma(n_cell),
            dma(n_cell),
            dma(n_gene),
            dma(n_gene),
            dma(devices),
            dma(devices),
            dma(n_cell),
            dma(n_cell),
            pltpu.SemaphoreType.DMA,
        ],
        compiler_params=pltpu.CompilerParams(
            collective_id=0, has_side_effects=True, vmem_limit_bytes=60 * 1024 * 1024
        ),
    )(counts, totals.reshape(1, cells), cell_factors.T, gene_loadings.T)
    return (new_factors.T, new_loadings.T, deviance.reshape(genes))


def solution(mesh):
    n_cell, n_gene = mesh.shape["cell"], mesh.shape["gene"]

    def on_device(counts, totals, cell_factors, gene_loadings):
        cells, genes = counts.shape
        whole_lanes = genes == n_cell * LANES and 2 * cells == n_gene * LANES
        if whole_lanes and n_gene % 2 == 0 and genes % BLOCK == 0:
            return by_kernel(n_cell, n_gene, counts, totals, cell_factors, gene_loadings)
        return by_collectives(counts, totals, cell_factors, gene_loadings)

    return jax.shard_map(
        on_device,
        mesh=mesh,
        in_specs=(P("cell", "gene"), P("cell"), P("cell", None), P("gene", None)),
        out_specs=(P("cell", None), P("gene", None), P("gene")),
        check_vma=False,
    )
```
